32 devices in a mesh: views: 8 (over z, y), rows: 4 (over x, core).
Axes of the slice: x: 2, y: 2, z: 4, core: 2. Of those that a mesh axis runs over, the one named last changes fastest.
Arguments:
- sinogram: bfloat16 [8, 64, 2048], P(None, 'views'), may hold values from -32 to 6176
- view_shift: int32 [64], P('views'), may hold values from -48 to 48
- conv_one: float32 [9, 32], replicated, may hold values from -2 to 2
- bias_one: float32 [32], replicated, may hold values from -3 to 3
- conv_two: bfloat16 [32, 288], replicated, may hold values from -0.375 to 0.375
- bias_two: float32 [32], replicated, may hold values from -3 to 3
Outputs:
- denoised: bfloat16 [8, 32, 16, 2048], P('views', None, 'rows')
The draws below stay inside these ranges and needn't reach their ends.
All inputs are finite; a program needn't handle non-finite values.
Results may differ from the reference program's by a relative error of at most 0.008.
Values may be sent and summed in bfloat16 or wider, within the bound.
A program may use at most 64 MiB of HBM per device.

```python
import math
import jax
import jax.numpy as jnp
from jax import lax

BINS = 2048
WIDTH = 2048
CHAN = 32
MARGIN = 384
SHIFT_MAX = 48
VIEWS = 64
SLICES = 8
IMG_ROWS = 16


def draw_sinogram(key, part):
    radius = WIDTH / 2.0
    angle = jnp.arange(VIEWS, dtype=jnp.float32) * (math.pi / VIEWS)
    cosine = jnp.cos(angle)[None, :, None]
    sine = jnp.sin(angle)[None, :, None]
    detector = (jnp.arange(BINS, dtype=jnp.float32) - (BINS - 1) / 2.0)[None, None, :]
    count = 4
    dense_low = 0.2
    dense_high = 1.0
    axis_low = 0.15
    axis_high = 0.5
    keys = jax.random.split(key, 7)
    shape = (SLICES, count)
    centre_x = jax.random.uniform(keys[0], shape, jnp.float32, -0.5, 0.5) * radius
    centre_y = jax.random.uniform(keys[1], shape, jnp.float32, -0.3, 0.3) * radius
    semi_first = jax.random.uniform(keys[2], shape, jnp.float32, axis_low, axis_high) * radius
    semi_second = jax.random.uniform(keys[3], shape, jnp.float32, axis_low, axis_high) * radius
    tilt = jax.random.uniform(keys[4], shape, jnp.float32, 0.0, math.pi)
    density = jax.random.uniform(keys[5], shape, jnp.float32, dense_low, dense_high)
    total = jnp.zeros((SLICES, VIEWS, BINS), jnp.float32)
    for item in range(count):
        first = semi_first[:, item][:, None, None]
        second = semi_second[:, item][:, None, None]
        turned = angle[None, :, None] - tilt[:, item][:, None, None]
        reach_sq = (first * jnp.cos(turned)) ** 2 + (second * jnp.sin(turned)) ** 2
        offset = detector - (centre_x[:, item][:, None, None] * cosine + centre_y[:, item][:, None, None] * sine)
        chord = 2.0 * first * second / reach_sq * jnp.sqrt(jnp.maximum(reach_sq - offset * offset, 0.0))
        total = total + density[:, item][:, None, None] * chord
    noise = jnp.clip(6.0 * jax.random.normal(keys[6], (SLICES, VIEWS, BINS), jnp.float32), -30.0, 30.0)
    return (total + noise).astype(jnp.bfloat16)


def set_ends(drawn, stream_key, smallest, top_value):
    dims = drawn.shape
    place = [jax.random.randint(jax.random.fold_in(stream_key, axis), (), 0, dims[axis]) for axis in range(len(dims))]
    drawn = drawn.at[tuple(place)].set(smallest)
    longest = dims.index(max(dims))
    place[longest] = (place[longest] + 1) % dims[longest]
    return drawn.at[tuple(place)].set(top_value)


def centred(key, extent, deviation, most, held_as=jnp.bfloat16):
    entries = deviation * jax.random.normal(key, extent, jnp.float32)
    return jnp.clip(entries, min=-most, max=most).astype(held_as)


def setup_inputs(seed: int = 0) -> dict:
    seeds = jax.random.split(jax.random.key(seed), 7)
    return {
        "sinogram": draw_sinogram(jax.random.fold_in(seeds[6], 71), 0),
        "view_shift": set_ends(jax.random.randint(seeds[1], (VIEWS,), 0 - SHIFT_MAX, SHIFT_MAX + 1), jax.random.fold_in(seeds[1], 1), 0 - SHIFT_MAX, SHIFT_MAX).astype(jnp.int32),
        "conv_one": centred(seeds[2], (9, CHAN), 9 ** -0.5, 2.0, jnp.float32),
        "bias_one": centred(seeds[3], (CHAN,), 0.5, 3.0, jnp.float32),
        "conv_two": centred(seeds[4], (CHAN, 9 * CHAN), (9 * CHAN) ** -0.5, 0.375),
        "bias_two": centred(seeds[5], (CHAN,), 0.5, 3.0, jnp.float32),
    }


def ramp_table(detector):
    indices = jnp.arange(detector, dtype=jnp.int32)
    offset = indices[None, :] - indices[:, None]
    square = (offset * offset).astype(jnp.float32)
    guarded = jnp.maximum(square, 1.0)
    is_odd = (offset % 2) != 0
    values = jnp.where(offset == 0, 0.25, jnp.where(is_odd, -1.0 / ((math.pi * math.pi) * guarded), 0.0))
    return values.astype(jnp.float32)


def filter_views(sinogram):
    sheets, view_count, detector = sinogram.shape
    table = ramp_table(detector)
    flat = sinogram.reshape(sheets * view_count, detector).astype(jnp.float32)
    result = jnp.dot(flat, table, precision=lax.Precision.HIGHEST, preferred_element_type=jnp.float32)
    return result.astype(jnp.bfloat16).reshape(sheets, view_count, detector)


def first_layer(extended, conv_one, bias_one):
    row_count = extended.shape[1] - 2
    columns = extended.shape[2]
    padded = jnp.pad(extended.astype(jnp.float32), ((0, 0), (0, 0), (1, 1)))
    running = jnp.zeros((extended.shape[0], conv_one.shape[1], row_count, columns), jnp.float32)
    running = running + bias_one[None, :, None, None]
    for kernel_tap in range(9):
        row_off = kernel_tap // 3
        col_off = kernel_tap % 3
        window = padded[:, row_off:row_off + row_count, col_off:col_off + columns]
        running = running + conv_one[kernel_tap][None, :, None, None] * window[:, None]
    return jnp.maximum(running, 0.0).astype(jnp.bfloat16)


def second_layer(extended, conv_two, bias_two):
    sheets, channels, rows_ext, columns = extended.shape
    row_count = rows_ext - 2
    padded = jnp.pad(extended, ((0, 0), (0, 0), (0, 0), (1, 1)))
    windows = [padded[:, :, kernel_tap // 3:kernel_tap // 3 + row_count, kernel_tap % 3:kernel_tap % 3 + columns] for kernel_tap in range(9)]
    stacked = jnp.stack(windows, axis=1).reshape(sheets, 9 * channels, row_count * columns)
    mixed = jnp.einsum("ok,skn->son", conv_two.astype(jnp.float32), stacked.astype(jnp.float32), precision=lax.Precision.HIGHEST)
    mixed = mixed + bias_two[None, :, None]
    return jnp.maximum(mixed, 0.0).astype(jnp.bfloat16).reshape(sheets, channels, row_count, columns)


def reference(sinogram, view_shift, conv_one, bias_one, conv_two, bias_two):
    filtered = filter_views(sinogram)
    padded = jnp.pad(filtered, ((0, 0), (0, 0), (MARGIN, MARGIN)))
    sheets_by_view = jnp.swapaxes(padded, 0, 1)
    columns = jnp.arange(WIDTH, dtype=jnp.float32) - (WIDTH - 1) / 2.0
    rows_y = jnp.arange(IMG_ROWS, dtype=jnp.int32).astype(jnp.float32) - (IMG_ROWS - 1) / 2.0

    def one_view(running, inputs):
        view_index, shift, sheet = inputs
        angle = view_index.astype(jnp.float32) * (math.pi / VIEWS)
        cosine = jnp.cos(angle)
        sine = jnp.sin(angle)
        center = shift.astype(jnp.float32) + ((BINS - 1) / 2.0 + MARGIN)
        position = (columns[None, :] * cosine + rows_y[:, None] * sine) + center
        lower = jnp.floor(position)
        lower_index = lower.astype(jnp.int32)
        weight_low = jnp.maximum(0.0, 1.0 - jnp.abs(position - lower)).astype(jnp.bfloat16)
        weight_high = jnp.maximum(0.0, 1.0 - jnp.abs(position - (lower + 1.0))).astype(jnp.bfloat16)
        low_values = jnp.take(sheet, lower_index, axis=1).astype(jnp.float32)
        high_values = jnp.take(sheet, lower_index + 1, axis=1).astype(jnp.float32)
        term = low_values * weight_low.astype(jnp.float32)[None] + high_values * weight_high.astype(jnp.float32)[None]
        return running + term, 0

    start = jnp.zeros((SLICES, IMG_ROWS, WIDTH), jnp.float32)
    running = lax.scan(one_view, start, (jnp.arange(VIEWS, dtype=jnp.int32), view_shift, sheets_by_view))[0]
    image = (running * (math.pi / VIEWS)).astype(jnp.bfloat16)

    def one_slice(sheet):
        extended = jnp.pad(sheet[None], ((0, 0), (1, 1), (0, 0)))
        hidden = first_layer(extended, conv_one, bias_one)
        hidden = jnp.pad(hidden, ((0, 0), (0, 0), (1, 1), (0, 0)))
        return second_layer(hidden, conv_two, bias_two)[0]

    return lax.map(one_slice, image)
```

```python
import functools
import math

import jax
import jax.numpy as jnp
import numpy as np
from jax import lax
from jax.experimental import pallas as pl
from jax.experimental.pallas import tpu as pltpu
from jax.sharding import PartitionSpec as P

MARGIN = 384
ROW_DEV = 4
LANES = 128
BLOCK = 256
QUARTERS = 4
F32 = jnp.float32
BF16 = jnp.bfloat16
MESH = pl.DeviceIdType.MESH


def split_parts(values, count):
    parts = []
    rest = values
    for part in range(count):
        piece = rest.astype(BF16)
        parts.append(piece)
        if part + 1 < count:
            rest = rest - piece.astype(F32)
    return parts


def ramp_block(block_offset):
    rows = lax.broadcasted_iota(jnp.int32, (BLOCK, BLOCK), 0)
    cols = lax.broadcasted_iota(jnp.int32, (BLOCK, BLOCK), 1)
    offset = cols - rows + block_offset * BLOCK
    square = (offset * offset).astype(F32)
    taps = jnp.where((offset & 1) != 0, (-1.0 / (math.pi * math.pi)) / jnp.maximum(square, 1.0), 0.0)
    if block_offset == 0:
        taps = jnp.where(offset == 0, 0.25, taps)
    return taps


def dot(a, b):
    return lax.dot_general(a, b, (((1,), (0,)), ((), ())), preferred_element_type=F32)


def dot_t(a, b):
    return lax.dot_general(a, b, (((1,), (1,)), ((), ())), preferred_element_type=F32)


def project_kernel(views_total, image_rows, sino_ref, perm_in_ref, perm_out_ref, shift_ref, cos_ref, sin_ref,
                   out_ref, sum_ref, low_ref, high_ref, part_ref):
    slices, view_count, bins = sino_ref.shape
    width = bins
    flat = slices * view_count
    blocks = bins // BLOCK
    ordered = dot(perm_in_ref[...], sino_ref[...].reshape(flat, bins)).astype(BF16)
    stacked = jnp.concatenate([ordered[:, k * BLOCK:(k + 1) * BLOCK] for k in range(blocks)], axis=0)
    for step in range(blocks):
        parts = split_parts(ramp_block(step), 3 if step < 2 else 2)
        count = (blocks - step) * flat
        down = stacked[:count]
        forward = sum(dot(down, part) for part in parts[::-1])
        if step == 0:
            sum_ref[...] = forward
        else:
            sum_ref[pl.ds(step * flat, count), :] += forward
            up = stacked[step * flat:]
            backward = sum(dot_t(up, part) for part in parts[::-1])
            sum_ref[pl.ds(0, count), :] += backward
    extended = low_ref.shape[1]
    low_ref[:, :MARGIN] = jnp.zeros((flat, MARGIN), F32)
    low_ref[:, MARGIN + bins:] = jnp.zeros((flat, extended - MARGIN - bins), F32)
    for k in range(blocks):
        low_ref[:, MARGIN + k * BLOCK:MARGIN + (k + 1) * BLOCK] = (
            sum_ref[k * flat:(k + 1) * flat, :].astype(BF16).astype(F32)
        )
    high_ref[...] = pltpu.roll(low_ref[...], extended - 1, 1)

    first_view = lax.axis_index("views") * view_count
    row_base = lax.axis_index("rows") * ROW_DEV
    half = (width - 1) / 2.0
    lanes = lax.broadcasted_iota(jnp.int32, (slices, LANES), 1).astype(F32)

    def tile(index, carry):
        base = (index * LANES).astype(F32) - half
        x_all = lanes + base
        totals = [jnp.zeros((slices, LANES), F32) for _ in range(ROW_DEV)]
        for view in range(view_count):
            cosine = cos_ref[first_view + view]
            sine = sin_ref[first_view + view]
            center = shift_ref[view].astype(F32) + ((bins - 1) / 2.0 + MARGIN)
            along = x_all * cosine
            ends = jnp.minimum(base * cosine, (base + (LANES - 1.0)) * cosine)
            for row in range(ROW_DEV):
                y = (row_base + row).astype(F32) - (image_rows - 1) / 2.0
                lift = y * sine
                place = (along + lift) + center
                block = ((ends + lift + center - 0.01) * (1.0 / LANES)).astype(jnp.int32)
                start = pl.multiple_of(block * LANES, LANES)
                lower = jnp.floor(place)
                fraction = place - lower
                weight_low = (1.0 - fraction).astype(BF16).astype(F32)
                weight_high = fraction.astype(BF16).astype(F32)
                spot = lower.astype(jnp.int32) - start
                near = spot < LANES
                inner = spot & (LANES - 1)
                rows = slice(view * slices, (view + 1) * slices)
                take = functools.partial(jnp.take_along_axis, indices=inner, axis=1, mode="promise_in_bounds")
                after = pl.multiple_of(start + LANES, LANES)
                low = jnp.where(near, take(low_ref[rows, pl.ds(start, LANES)]),
                                take(low_ref[rows, pl.ds(after, LANES)]))
                high = jnp.where(near, take(high_ref[rows, pl.ds(start, LANES)]),
                                 take(high_ref[rows, pl.ds(after, LANES)]))
                totals[row] = totals[row] + (low * weight_low + high * weight_high)
        for row in range(ROW_DEV):
            part_ref[row * slices:(row + 1) * slices, pl.ds(pl.multiple_of(index * LANES, LANES), LANES)] = totals[row]
        return carry

    lax.fori_loop(0, width // LANES, tile, 0)
    span = width // QUARTERS
    gathered = jnp.concatenate([part_ref[:, q * span:(q + 1) * span] for q in range(QUARTERS)], axis=0).astype(BF16)
    out_ref[...] = dot(perm_out_ref[...], gathered).astype(BF16).reshape(out_ref.shape)


def exchange_kernel(views, row_groups, scale, part_ref, out_ref, recv_ref, own_ref, up_ref, down_ref,
                    send_sem, recv_sem, halo_send, halo_recv):
    me = lax.axis_index("views")
    group = lax.axis_index("rows")
    above = lax.rem(group + row_groups - 1, row_groups)
    below = lax.rem(group + 1, row_groups)
    barrier = pltpu.get_barrier_semaphore()
    for step in range(1, views):
        pl.semaphore_signal(barrier, inc=1, device_id={"views": lax.rem(me + step, views)}, device_id_type=MESH)
    for other in (above, below):
        pl.semaphore_signal(barrier, inc=1, device_id={"rows": other}, device_id_type=MESH)
    pl.semaphore_wait(barrier, views + 1)
    group_slices = part_ref.shape[0] // views
    copies = []
    for step in range(1, views):
        peer = lax.rem(me + step, views)
        copy = pltpu.make_async_remote_copy(
            src_ref=part_ref.at[pl.ds(peer * group_slices, group_slices)], dst_ref=recv_ref.at[step - 1],
            send_sem=send_sem.at[step - 1], recv_sem=recv_sem.at[step - 1],
            device_id={"views": peer}, device_id_type=MESH)
        copy.start()
        copies.append(copy)
    total = part_ref[pl.ds(me * group_slices, group_slices)].astype(F32)
    for step, copy in enumerate(copies):
        copy.wait_recv()
        total = total + recv_ref[step].astype(F32)
    image = (total * scale).astype(BF16).astype(F32)
    own_ref[...] = image
    rows_half = own_ref.shape[1] // 2
    to_above = pltpu.make_async_remote_copy(
        src_ref=own_ref.at[:, pl.ds(0, rows_half)], dst_ref=down_ref, send_sem=halo_send.at[0], recv_sem=halo_recv.at[0],
        device_id={"rows": above}, device_id_type=MESH)
    to_below = pltpu.make_async_remote_copy(
        src_ref=own_ref.at[:, pl.ds(rows_half, rows_half)], dst_ref=up_ref, send_sem=halo_send.at[1], recv_sem=halo_recv.at[1],
        device_id={"rows": below}, device_id_type=MESH)
    to_above.start()
    to_below.start()
    span = own_ref.shape[2]

    def place(index, values, first_row, count):
        for row in range(count):
            for q in range(QUARTERS):
                out_ref[index, first_row + row:first_row + row + 1, q * span:(q + 1) * span] = (
                    values[row * QUARTERS + q:row * QUARTERS + q + 1])

    for index in range(group_slices):
        place(index, image[index], 2, ROW_DEV)
    to_above.wait_recv()
    to_below.wait_recv()
    has_above = (group > 0).astype(F32)
    has_below = (group < row_groups - 1).astype(F32)
    for index in range(group_slices):
        place(index, up_ref[index] * has_above, 0, 2)
        place(index, down_ref[index] * has_below, 2 + ROW_DEV, 2)
    for copy in copies + [to_above, to_below]:
        copy.wait_send()


def conv_kernel(row_groups, rows_ref, one_ref, bias_one_ref, two_ref, bias_two_ref, out_ref):
    group = lax.axis_index("rows")
    width = rows_ref.shape[2]
    channels = out_ref.shape[1]
    source = rows_ref[0]
    column = lax.broadcasted_iota(jnp.int32, (1, width), 1)

    def spread(values):
        left = jnp.where(column == 0, 0.0, pltpu.roll(values, 1, 1))
        right = jnp.where(column == width - 1, 0.0, pltpu.roll(values, width - 1, 1))
        return [left, values, right]

    window = jnp.concatenate(spread(source), axis=0).astype(BF16)
    window = jnp.concatenate([window] * 3, axis=0)
    hidden = jnp.maximum(dot(one_ref[...], window) + bias_one_ref[...], 0.0)
    hidden_rows = ROW_DEV + 2
    line = lax.broadcasted_iota(jnp.int32, (hidden_rows * channels, 1), 0)
    lowest = jnp.where(group > 0, 0, channels)
    highest = jnp.where(group < row_groups - 1, hidden_rows * channels, (hidden_rows - 1) * channels)
    hidden = jnp.where((line >= lowest) & (line < highest), hidden, 0.0)
    stacked = jnp.concatenate([piece.astype(BF16) for piece in spread(hidden)], axis=0)
    mixed = jnp.maximum(dot(two_ref[...], stacked) + bias_two_ref[...], 0.0)
    out_ref[0] = mixed.reshape(channels, ROW_DEV, width).astype(BF16)


def spread_one(conv_one):
    channels = conv_one.shape[1]
    hidden_rows = ROW_DEV + 2
    taps = conv_one.reshape(3, 3, channels).transpose(2, 1, 0)
    rows = [jnp.pad(taps, ((0, 0), (0, 0), (r, hidden_rows - 1 - r))) for r in range(hidden_rows)]
    full = jnp.stack(rows, axis=0).reshape(hidden_rows * channels, 3 * (hidden_rows + 2))
    return jnp.concatenate(split_parts(full, 3), axis=1)


def spread_two(conv_two):
    channels = conv_two.shape[0]
    taps = conv_two.reshape(channels, 3, 3, channels).transpose(0, 2, 1, 3)
    rows = [jnp.pad(taps, ((0, 0), (0, 0), (r, ROW_DEV - 1 - r), (0, 0))) for r in range(ROW_DEV)]
    return jnp.stack(rows, axis=1).reshape(channels * ROW_DEV, 3 * (ROW_DEV + 2) * channels)


def local(sinogram, view_shift, conv_one, bias_one, conv_two, bias_two):
    slices, view_count, bins = sinogram.shape
    views = lax.axis_size("views")
    row_groups = lax.axis_size("rows")
    views_total = view_count * views
    image_rows = ROW_DEV * row_groups
    channels = conv_one.shape[1]
    flat = slices * view_count
    group_slices = slices // views
    extended = bins + 2 * MARGIN
    span = bins // QUARTERS

    angles = (np.arange(views_total, dtype=np.float32) * np.float32(math.pi / views_total)).astype(np.float64)
    cosines = jnp.asarray(np.cos(angles).astype(np.float32))
    sines = jnp.asarray(np.sin(angles).astype(np.float32))
    order = np.arange(flat).reshape(slices, view_count).T.reshape(-1)
    perm_in = np.zeros((flat, flat), np.float32)
    perm_in[np.arange(flat), order] = 1.0
    size = QUARTERS * ROW_DEV * slices
    order = np.arange(size).reshape(QUARTERS, ROW_DEV, slices).transpose(2, 1, 0).reshape(-1)
    perm_out = np.zeros((size, size), np.float32)
    perm_out[np.arange(size), order] = 1.0

    vmem = pl.BlockSpec(memory_space=pltpu.VMEM)
    smem = pl.BlockSpec(memory_space=pltpu.SMEM)
    partial = pl.pallas_call(
        functools.partial(project_kernel, views_total, image_rows),
        out_shape=jax.ShapeDtypeStruct((slices, QUARTERS * ROW_DEV, span), BF16),
        in_specs=[vmem] * 3 + [smem] * 3,
        out_specs=vmem,
        scratch_shapes=[
            pltpu.VMEM((bins // BLOCK * flat, BLOCK), F32),
            pltpu.VMEM((flat, extended), F32),
            pltpu.VMEM((flat, extended), F32),
            pltpu.VMEM((ROW_DEV * slices, bins), F32),
        ],
        name="project",
    )(sinogram, jnp.asarray(perm_in, dtype=BF16), jnp.asarray(perm_out, dtype=BF16), view_shift, cosines, sines)

    halo = pltpu.VMEM((group_slices, QUARTERS * ROW_DEV // 2, span), F32)
    rows = pl.pallas_call(
        functools.partial(exchange_kernel, views, row_groups, math.pi / views_total),
        out_shape=jax.ShapeDtypeStruct((group_slices, ROW_DEV + 4, bins), F32),
        in_specs=[vmem],
        out_specs=vmem,
        scratch_shapes=[
            pltpu.VMEM((views - 1, group_slices, QUARTERS * ROW_DEV, span), BF16),
            pltpu.VMEM((group_slices, QUARTERS * ROW_DEV, span), F32),
            halo,
            halo,
            pltpu.SemaphoreType.DMA((views - 1,)),
            pltpu.SemaphoreType.DMA((views - 1,)),
            pltpu.SemaphoreType.DMA((2,)),
            pltpu.SemaphoreType.DMA((2,)),
        ],
        compiler_params=pltpu.CompilerParams(collective_id=0, has_side_effects=True),
        name="exchange",
    )(partial)

    hidden_rows = ROW_DEV + 2
    one = spread_one(conv_one)
    two = spread_two(conv_two)
    one_bias = jnp.tile(bias_one, hidden_rows)[:, None]
    two_bias = jnp.repeat(bias_two, ROW_DEV)[:, None]
    conv = pl.pallas_call(
        functools.partial(conv_kernel, row_groups),
        grid=(group_slices,),
        out_shape=jax.ShapeDtypeStruct((group_slices, channels, ROW_DEV, bins), BF16),
        in_specs=[pl.BlockSpec((1, ROW_DEV + 4, bins), lambda i: (i, 0, 0))] + [vmem] * 4,
        out_specs=pl.BlockSpec((1, channels, ROW_DEV, bins), lambda i: (i, 0, 0, 0)),
        name="conv",
    )
    return conv(rows, one, one_bias, two, two_bias)


def solution(mesh):
    return jax.shard_map(
        local,
        mesh=mesh,
        in_specs=(P(None, "views", None), P("views"), P(), P(), P(), P()),
        out_specs=P("views", None, "rows", None),
        check_vma=False,
    )
```

```python
import functools
import math

import jax
import jax.numpy as jnp
import numpy as np
from jax import lax
from jax.experimental import pallas as pl
from jax.experimental.pallas import tpu as pltpu
from jax.sharding import PartitionSpec as P

MARGIN = 384
ROW_DEV = 4
LANES = 128
BLOCK = 256
QUARTERS = 4
CHUNKS = 2
FIXED = 18
F32 = jnp.float32
BF16 = jnp.bfloat16
MESH = pl.DeviceIdType.MESH


def split_parts(values, count):
    parts = []
    rest = values
    for part in range(count):
        piece = rest.astype(BF16)
        parts.append(piece)
        if part + 1 < count:
            rest = rest - piece.astype(F32)
    return parts


def ramp_block(block_offset):
    rows = lax.broadcasted_iota(jnp.int32, (BLOCK, BLOCK), 0)
    cols = lax.broadcasted_iota(jnp.int32, (BLOCK, BLOCK), 1)
    offset = cols - rows + block_offset * BLOCK
    square = (offset * offset).astype(F32)
    taps = jnp.where((offset & 1) != 0, (-1.0 / (math.pi * math.pi)) / jnp.maximum(square, 1.0), 0.0)
    if block_offset == 0:
        taps = jnp.where(offset == 0, 0.25, taps)
    return taps


def dot(a, b):
    return lax.dot_general(a, b, (((1,), (0,)), ((), ())), preferred_element_type=F32)


def dot_t(a, b):
    return lax.dot_general(a, b, (((1,), (1,)), ((), ())), preferred_element_type=F32)


def tap_matrices(one_ref, bias_one_ref, two_ref, bias_two_ref, expand_ref):
    channels = one_ref.shape[1]
    hidden_rows = ROW_DEV + 2
    image_lines = ROW_DEV + 4
    lanes = hidden_rows * channels
    rep = jnp.concatenate([one_ref[...]] * hidden_rows, axis=1)
    line = lax.broadcasted_iota(jnp.int32, (3 * image_lines, lanes), 0) % image_lines
    target = lax.broadcasted_iota(jnp.int32, (3 * image_lines, lanes), 1) // channels
    full = jnp.zeros((3 * image_lines, lanes), F32)
    for i in range(3):
        picked = jnp.concatenate(
            [jnp.broadcast_to(rep[3 * i + dx:3 * i + dx + 1], (image_lines, lanes)) for dx in range(3)], axis=0)
        full = full + jnp.where(line - target == i, picked, 0.0)
    bias = jnp.concatenate([bias_one_ref[...]] * hidden_rows, axis=1)
    bias_parts = [piece.astype(F32) for piece in split_parts(bias, 3)]
    bias_rows = jnp.concatenate(bias_parts + [jnp.zeros((5, lanes), F32)], axis=0)
    pieces = [piece.astype(F32) for piece in split_parts(full, 3)]
    one = jnp.concatenate(pieces + [bias_rows], axis=0).T.astype(BF16)
    taps = two_ref[...].astype(F32)
    depth = 3 * hidden_rows * channels
    rows = channels * ROW_DEV
    out_row = lax.broadcasted_iota(jnp.int32, (rows, depth), 0) % ROW_DEV
    hidden_row = (lax.broadcasted_iota(jnp.int32, (rows, depth), 1) // channels) % hidden_rows
    two = jnp.zeros((rows, depth), F32)
    for i in range(3):
        wide = jnp.concatenate(
            [taps[:, (3 * i + dx) * channels:(3 * i + dx + 1) * channels] for dx in range(3) for _ in range(hidden_rows)],
            axis=1)
        two = two + jnp.where(hidden_row - out_row == i, dot(expand_ref[...], wide.astype(BF16)), 0.0)
    second = sum(dot_t(expand_ref[...], jnp.broadcast_to(piece.astype(F32), (LANES, channels)).astype(BF16))
                 for piece in split_parts(bias_two_ref[...], 3))
    return one, two.astype(BF16), second


def project_kernel(views, row_groups, sino_ref, perm_in_ref, perm_out_ref, expand_ref, shift_ref, cos_ref, sin_ref, fixed_cos_ref, fixed_sin_ref,
                   conv_one_ref, bias_one_ref, conv_two_ref, bias_two_ref,
                   out_ref, one_ref, two_ref, second_ref,
                   sum_ref, low_ref, high_ref, part_ref, send_ref, recv_ref, own_ref, up_ref, down_ref,
                   send_sem, recv_sem, halo_send, halo_recv):
    me = lax.axis_index("views")
    group = lax.axis_index("rows")
    above = lax.rem(group + row_groups - 1, row_groups)
    below = lax.rem(group + 1, row_groups)
    barrier = pltpu.get_barrier_semaphore()
    for step in range(1, views):
        pl.semaphore_signal(barrier, inc=1, device_id={"views": lax.rem(me + step, views)}, device_id_type=MESH)
    for other in (above, below):
        pl.semaphore_signal(barrier, inc=1, device_id={"rows": other}, device_id_type=MESH)

    slices, view_count, bins = sino_ref.shape
    width = bins
    flat = slices * view_count
    blocks = bins // BLOCK
    views_total = view_count * views
    image_rows = ROW_DEV * row_groups
    scale = math.pi / views_total
    ordered = dot(perm_in_ref[...], sino_ref[...].reshape(flat, bins)).astype(BF16)
    stacked = jnp.concatenate([ordered[:, k * BLOCK:(k + 1) * BLOCK] for k in range(blocks)], axis=0)
    for step in range(blocks):
        parts = split_parts(ramp_block(step), 3 if step < 2 else 2)
        count = (blocks - step) * flat
        down = stacked[:count]
        forward = sum(dot(down, part) for part in parts[::-1])
        if step == 0:
            sum_ref[...] = forward
        else:
            sum_ref[pl.ds(step * flat, count), :] += forward
            up = stacked[step * flat:]
            backward = sum(dot_t(up, part) for part in parts[::-1])
            sum_ref[pl.ds(0, count), :] += backward
    zeros = jnp.zeros((flat, MARGIN), F32)
    filtered = [sum_ref[k * flat:(k + 1) * flat, :].astype(BF16).astype(F32) for k in range(blocks)]
    padded = jnp.concatenate([zeros] + filtered + [zeros], axis=1)
    shifted = pltpu.roll(padded, padded.shape[1] - 1, 1)
    for block in range(low_ref.shape[0]):
        low_ref[block] = padded[:, block * LANES:(block + 1) * LANES]
        high_ref[block] = shifted[:, block * LANES:(block + 1) * LANES]

    first_view = me * view_count
    row_base = group * ROW_DEV
    half = (width - 1) / 2.0
    lanes = lax.broadcasted_iota(jnp.int32, (slices, LANES), 1).astype(F32)
    chunk_cols = width // CHUNKS
    fixed_half = (1 << FIXED) - (1 << (FIXED - 4))
    span = chunk_cols // QUARTERS
    group_slices = slices // views

    def tile(chunk, index, carry):
        base = (index * LANES + chunk * chunk_cols).astype(F32) - half
        x_all = lanes + base
        twice_base = 2 * (index * LANES + chunk * chunk_cols) - (width - 1)
        totals = [jnp.zeros((slices, LANES), F32) for _ in range(ROW_DEV)]
        for view in range(view_count):
            cosine = cos_ref[first_view + view]
            sine = sin_ref[first_view + view]
            center = shift_ref[view].astype(F32) + ((bins - 1) / 2.0 + MARGIN)
            along = x_all * cosine
            fixed_cos = fixed_cos_ref[first_view + view]
            fixed_sin = fixed_sin_ref[first_view + view]
            ends = jnp.minimum(twice_base * fixed_cos, (twice_base + 2 * (LANES - 1)) * fixed_cos) + fixed_half
            origin = shift_ref[view] + ((bins - 1) // 2 + MARGIN)
            for row in range(ROW_DEV):
                y = (row_base + row).astype(F32) - (image_rows - 1) / 2.0
                lift = y * sine
                place = (along + lift) + center
                twice_y = 2 * (row_base + row) - (image_rows - 1)
                lowest = ((ends + twice_y * fixed_sin) >> (FIXED + 1)) + origin
                block = lowest >> 7
                lower = jnp.floor(place)
                fraction = place - lower
                weight_low = (1.0 - fraction).astype(BF16).astype(F32)
                weight_high = fraction.astype(BF16).astype(F32)
                spot = lower.astype(jnp.int32) - block * LANES
                near = spot < LANES
                inner = spot & (LANES - 1)
                rows = slice(view * slices, (view + 1) * slices)
                take = functools.partial(jnp.take_along_axis, indices=inner, axis=1, mode="promise_in_bounds")
                low = jnp.where(near, take(low_ref[block, rows]), take(low_ref[block + 1, rows]))
                high = jnp.where(near, take(high_ref[block, rows]), take(high_ref[block + 1, rows]))
                totals[row] = totals[row] + (low * weight_low + high * weight_high)
        for row in range(ROW_DEV):
            part_ref[row * slices:(row + 1) * slices, pl.ds(pl.multiple_of(index * LANES, LANES), LANES)] = totals[row]
        return carry

    copies = []
    for chunk in range(CHUNKS):
        lax.fori_loop(0, chunk_cols // LANES, functools.partial(tile, chunk), 0)
        gathered = jnp.concatenate([part_ref[:, q * span:(q + 1) * span] for q in range(QUARTERS)], axis=0).astype(BF16)
        send_ref[chunk] = dot(perm_out_ref[...], gathered).astype(BF16).reshape(slices, QUARTERS * ROW_DEV, span)
        if chunk == 0:
            pl.semaphore_wait(barrier, views + 1)
        sent = []
        for step in range(1, views):
            peer = lax.rem(me + step, views)
            slot = chunk * (views - 1) + step - 1
            copy = pltpu.make_async_remote_copy(
                src_ref=send_ref.at[chunk, pl.ds(peer * group_slices, group_slices)], dst_ref=recv_ref.at[slot],
                send_sem=send_sem.at[slot], recv_sem=recv_sem.at[slot],
                device_id={"views": peer}, device_id_type=MESH)
            copy.start()
            sent.append((slot, copy))
        copies.append(sent)

    one, two, second = tap_matrices(conv_one_ref, bias_one_ref, conv_two_ref, bias_two_ref, expand_ref)
    one_ref[...] = one
    two_ref[...] = two
    second_ref[...] = second

    def place_rows(index, chunk, values, first_row, count):
        for row in range(count):
            for q in range(QUARTERS):
                column = chunk * chunk_cols + q * span
                out_ref[index, first_row + row:first_row + row + 1, column:column + span] = (
                    values[row * QUARTERS + q:row * QUARTERS + q + 1])

    rows_half = QUARTERS * ROW_DEV // 2
    halos = []
    for chunk in range(CHUNKS):
        total = send_ref[chunk, pl.ds(me * group_slices, group_slices)].astype(F32)
        for slot, copy in copies[chunk]:
            copy.wait_recv()
            total = total + recv_ref[slot].astype(F32)
        image = (total * scale).astype(BF16).astype(F32)
        own_ref[chunk] = image
        to_above = pltpu.make_async_remote_copy(
            src_ref=own_ref.at[chunk, :, pl.ds(0, rows_half)], dst_ref=down_ref.at[chunk],
            send_sem=halo_send.at[2 * chunk], recv_sem=halo_recv.at[2 * chunk],
            device_id={"rows": above}, device_id_type=MESH)
        to_below = pltpu.make_async_remote_copy(
            src_ref=own_ref.at[chunk, :, pl.ds(rows_half, rows_half)], dst_ref=up_ref.at[chunk],
            send_sem=halo_send.at[2 * chunk + 1], recv_sem=halo_recv.at[2 * chunk + 1],
            device_id={"rows": below}, device_id_type=MESH)
        to_above.start()
        to_below.start()
        halos.append((to_above, to_below))
        for index in range(group_slices):
            place_rows(index, chunk, image[index], 2, ROW_DEV)
    has_above = (group > 0).astype(F32)
    has_below = (group < row_groups - 1).astype(F32)
    for chunk, (to_above, to_below) in enumerate(halos):
        to_above.wait_recv()
        to_below.wait_recv()
        for index in range(group_slices):
            place_rows(index, chunk, up_ref[chunk, index] * has_above, 0, 2)
            place_rows(index, chunk, down_ref[chunk, index] * has_below, 2 + ROW_DEV, 2)
    for sent in copies:
        for _, copy in sent:
            copy.wait_send()
    for pair in halos:
        for copy in pair:
            copy.wait_send()


def conv_kernel(row_groups, rows_ref, one_ref, two_ref, second_ref, out_ref):
    group = lax.axis_index("rows")
    width = rows_ref.shape[2]
    channels = out_ref.shape[1]
    source = rows_ref[0]
    column = lax.broadcasted_iota(jnp.int32, (1, width), 1)

    def spread(values):
        left = jnp.where(column == 0, 0.0, pltpu.roll(values, 1, 1))
        right = jnp.where(column == width - 1, 0.0, pltpu.roll(values, width - 1, 1))
        return [left, values, right]

    window = jnp.concatenate(spread(source), axis=0).astype(BF16)
    window = jnp.concatenate([window] * 3 + [jnp.ones((8, width), BF16)], axis=0)
    hidden = jnp.maximum(dot(one_ref[...], window), 0.0)
    hidden_rows = ROW_DEV + 2
    line = lax.broadcasted_iota(jnp.int32, (hidden_rows * channels, 1), 0)
    lowest = jnp.where(group > 0, 0, channels)
    highest = jnp.where(group < row_groups - 1, hidden_rows * channels, (hidden_rows - 1) * channels)
    hidden = jnp.where((line >= lowest) & (line < highest), hidden, 0.0)
    stacked = jnp.concatenate([piece.astype(BF16) for piece in spread(hidden)], axis=0)
    mixed = jnp.maximum(dot(two_ref[...], stacked) + second_ref[:, :1], 0.0)
    out_ref[0] = mixed.reshape(channels, ROW_DEV, width).astype(BF16)


def local(sinogram, view_shift, conv_one, bias_one, conv_two, bias_two):
    slices, view_count, bins = sinogram.shape
    views = lax.axis_size("views")
    row_groups = lax.axis_size("rows")
    views_total = view_count * views
    image_rows = ROW_DEV * row_groups
    channels = conv_one.shape[1]
    flat = slices * view_count
    group_slices = slices // views
    extended = bins + 2 * MARGIN
    span = bins // (QUARTERS * CHUNKS)

    angles = (np.arange(views_total, dtype=np.float32) * np.float32(math.pi / views_total)).astype(np.float64)
    cosines = jnp.asarray(np.cos(angles).astype(np.float32))
    sines = jnp.asarray(np.sin(angles).astype(np.float32))
    fixed_cosines = jnp.asarray(np.round(np.cos(angles) * (1 << FIXED)).astype(np.int32))
    fixed_sines = jnp.asarray(np.round(np.sin(angles) * (1 << FIXED)).astype(np.int32))
    order = np.arange(flat).reshape(slices, view_count).T.reshape(-1)
    perm_in = np.zeros((flat, flat), np.float32)
    perm_in[np.arange(flat), order] = 1.0
    size = QUARTERS * ROW_DEV * slices
    order = np.arange(size).reshape(QUARTERS, ROW_DEV, slices).transpose(2, 1, 0).reshape(-1)
    perm_out = np.zeros((size, size), np.float32)
    perm_out[np.arange(size), order] = 1.0

    expand = np.repeat(np.eye(channels, dtype=np.float32), ROW_DEV, axis=0)

    vmem = pl.BlockSpec(memory_space=pltpu.VMEM)
    smem = pl.BlockSpec(memory_space=pltpu.SMEM)
    hidden_rows = ROW_DEV + 2
    halo = pltpu.VMEM((CHUNKS, group_slices, QUARTERS * ROW_DEV // 2, span), F32)
    slots = CHUNKS * (views - 1)
    rows, one, two, second = pl.pallas_call(
        functools.partial(project_kernel, views, row_groups),
        out_shape=(
            jax.ShapeDtypeStruct((group_slices, ROW_DEV + 4, bins), F32),
            jax.ShapeDtypeStruct((hidden_rows * channels, 9 * (ROW_DEV + 4) + 8), BF16),
            jax.ShapeDtypeStruct((channels * ROW_DEV, 3 * hidden_rows * channels), BF16),
            jax.ShapeDtypeStruct((channels * ROW_DEV, LANES), F32),
        ),
        in_specs=[vmem] * 4 + [smem] * 5 + [vmem] * 4,
        out_specs=(vmem,) * 4,
        scratch_shapes=[
            pltpu.VMEM((bins // BLOCK * flat, BLOCK), F32),
            pltpu.VMEM((extended // LANES, flat, LANES), F32),
            pltpu.VMEM((extended // LANES, flat, LANES), F32),
            pltpu.VMEM((ROW_DEV * slices, bins // CHUNKS), F32),
            pltpu.VMEM((CHUNKS, slices, QUARTERS * ROW_DEV, span), BF16),
            pltpu.VMEM((slots, group_slices, QUARTERS * ROW_DEV, span), BF16),
            pltpu.VMEM((CHUNKS, group_slices, QUARTERS * ROW_DEV, span), F32),
            halo,
            halo,
            pltpu.SemaphoreType.DMA((slots,)),
            pltpu.SemaphoreType.DMA((slots,)),
            pltpu.SemaphoreType.DMA((2 * CHUNKS,)),
            pltpu.SemaphoreType.DMA((2 * CHUNKS,)),
        ],
        compiler_params=pltpu.CompilerParams(collective_id=0, has_side_effects=True),
        name="project",
    )(sinogram, jnp.asarray(perm_in, dtype=BF16), jnp.asarray(perm_out, dtype=BF16), jnp.asarray(expand, dtype=BF16),
      view_shift, cosines, sines, fixed_cosines, fixed_sines, conv_one, bias_one[None, :], conv_two, bias_two[None, :])

    conv = pl.pallas_call(
        functools.partial(conv_kernel, row_groups),
        grid=(group_slices,),
        out_shape=jax.ShapeDtypeStruct((group_slices, channels, ROW_DEV, bins), BF16),
        in_specs=[pl.BlockSpec((1, ROW_DEV + 4, bins), lambda i: (i, 0, 0))] + [vmem] * 3,
        out_specs=pl.BlockSpec((1, channels, ROW_DEV, bins), lambda i: (i, 0, 0, 0)),
        name="conv",
    )
    return conv(rows, one, two, second)


def solution(mesh):
    return jax.shard_map(
        local,
        mesh=mesh,
        in_specs=(P(None, "views", None), P("views"), P(), P(), P(), P()),
        out_specs=P("views", None, "rows", None),
        check_vma=False,
    )
```

```python
import functools
import math

import jax
import jax.numpy as jnp
import numpy as np
from jax import lax
from jax.experimental import pallas as pl
from jax.experimental.pallas import tpu as pltpu
from jax.sharding import PartitionSpec as P

MARGIN = 384
ROW_DEV = 4
LANES = 128
BLOCK = 256
QUARTERS = 4
CHUNKS = 2
FIXED = 18
WINDOW = 64
F32 = jnp.float32
BF16 = jnp.bfloat16
MESH = pl.DeviceIdType.MESH


def split_parts(values, count):
    parts = []
    rest = values
    for part in range(count):
        piece = rest.astype(BF16)
        parts.append(piece)
        if part + 1 < count:
            rest = rest - piece.astype(F32)
    return parts


def ramp_base():
    rows = lax.broadcasted_iota(jnp.int32, (BLOCK, BLOCK), 0)
    cols = lax.broadcasted_iota(jnp.int32, (BLOCK, BLOCK), 1)
    offset = cols - rows
    return offset.astype(F32), jnp.where((offset & 1) != 0, -1.0 / (math.pi * math.pi), 0.0)


def ramp_block(base, numerator, block_offset):
    offset = base + float(block_offset * BLOCK)
    square = offset * offset
    if block_offset == 0:
        return jnp.where(base == 0.0, 0.25, numerator / jnp.maximum(square, 1.0))
    return numerator / square


def dot(a, b):
    return lax.dot_general(a, b, (((1,), (0,)), ((), ())), preferred_element_type=F32)


def dot_t(a, b):
    return lax.dot_general(a, b, (((1,), (1,)), ((), ())), preferred_element_type=F32)


def tap_matrices(one_ref, bias_one_ref, two_ref, bias_two_ref, expand_ref):
    channels = one_ref.shape[1]
    hidden_rows = ROW_DEV + 2
    image_lines = ROW_DEV + 4
    lanes = hidden_rows * channels
    rep = jnp.concatenate([one_ref[...]] * hidden_rows, axis=1)
    line = lax.broadcasted_iota(jnp.int32, (3 * image_lines, lanes), 0) % image_lines
    target = lax.broadcasted_iota(jnp.int32, (3 * image_lines, lanes), 1) // channels
    full = jnp.zeros((3 * image_lines, lanes), F32)
    for i in range(3):
        picked = jnp.concatenate(
            [jnp.broadcast_to(rep[3 * i + dx:3 * i + dx + 1], (image_lines, lanes)) for dx in range(3)], axis=0)
        full = full + jnp.where(line - target == i, picked, 0.0)
    bias = jnp.concatenate([bias_one_ref[...]] * hidden_rows, axis=1)
    bias_parts = [piece.astype(F32) for piece in split_parts(bias, 3)]
    bias_rows = jnp.concatenate(bias_parts + [jnp.zeros((5, lanes), F32)], axis=0)
    pieces = [piece.astype(F32) for piece in split_parts(full, 3)]
    one = jnp.concatenate(pieces + [bias_rows], axis=0).T.astype(BF16)
    taps = two_ref[...].astype(F32)
    depth = 3 * hidden_rows * channels
    rows = channels * ROW_DEV
    out_row = lax.broadcasted_iota(jnp.int32, (rows, depth), 0) % ROW_DEV
    hidden_row = (lax.broadcasted_iota(jnp.int32, (rows, depth), 1) // channels) % hidden_rows
    two = jnp.zeros((rows, depth), F32)
    for i in range(3):
        wide = jnp.concatenate(
            [taps[:, (3 * i + dx) * channels:(3 * i + dx + 1) * channels] for dx in range(3) for _ in range(hidden_rows)],
            axis=1)
        two = two + jnp.where(hidden_row - out_row == i, dot(expand_ref[...], wide.astype(BF16)), 0.0)
    second = sum(dot_t(expand_ref[...], jnp.broadcast_to(piece.astype(F32), (LANES, channels)).astype(BF16))
                 for piece in split_parts(bias_two_ref[...], 3))
    return one, two.astype(BF16), second


def project_kernel(views, row_groups, sino_ref, perm_in_ref, perm_out_ref, expand_ref, shift_ref, cos_ref, sin_ref, fixed_cos_ref, fixed_sin_ref,
                   conv_one_ref, bias_one_ref, conv_two_ref, bias_two_ref,
                   out_ref, one_ref, two_ref, second_ref,
                   sum_ref, low_ref, high_ref, part_ref, send_ref, recv_ref, own_ref, up_ref, down_ref,
                   send_sem, recv_sem, halo_send, halo_recv):
    me = lax.axis_index("views")
    group = lax.axis_index("rows")
    above = lax.rem(group + row_groups - 1, row_groups)
    below = lax.rem(group + 1, row_groups)
    barrier = pltpu.get_barrier_semaphore()
    for step in range(1, views):
        pl.semaphore_signal(barrier, inc=1, device_id={"views": lax.rem(me + step, views)}, device_id_type=MESH)
    for other in (above, below):
        pl.semaphore_signal(barrier, inc=1, device_id={"rows": other}, device_id_type=MESH)

    slices, view_count, bins = sino_ref.shape
    width = bins
    flat = slices * view_count
    blocks = bins // BLOCK
    views_total = view_count * views
    image_rows = ROW_DEV * row_groups
    scale = math.pi / views_total
    ordered = dot(perm_in_ref[...], sino_ref[...].reshape(flat, bins)).astype(BF16)
    stacked = jnp.concatenate([ordered[:, k * BLOCK:(k + 1) * BLOCK] for k in range(blocks)], axis=0)
    base_offset, numerator = ramp_base()
    for step in range(blocks):
        parts = split_parts(ramp_block(base_offset, numerator, step), 3 if step < 2 else 1)
        count = (blocks - step) * flat
        down = stacked[:count]
        forward = sum(dot(down, part) for part in parts[::-1])
        if step == 0:
            sum_ref[...] = forward
        else:
            sum_ref[pl.ds(step * flat, count), :] += forward
            up = stacked[step * flat:]
            backward = sum(dot_t(up, part) for part in parts[::-1])
            sum_ref[pl.ds(0, count), :] += backward
    zeros = jnp.zeros((flat, MARGIN), F32)
    filtered = [sum_ref[k * flat:(k + 1) * flat, :].astype(BF16).astype(F32) for k in range(blocks)]
    padded = jnp.concatenate([zeros] + filtered + [zeros], axis=1)
    for ref, lead in ((low_ref, 0), (high_ref, 1)):
        for odd in range(2):
            turn = odd * WINDOW + lead
            turned = pltpu.roll(padded, padded.shape[1] - turn, 1) if turn else padded
            for block in range(ref.shape[0] // 2):
                ref[2 * block + odd] = turned[:, block * LANES:(block + 1) * LANES]

    first_view = me * view_count
    row_base = group * ROW_DEV
    half = (width - 1) / 2.0
    lanes = lax.broadcasted_iota(jnp.int32, (slices, LANES), 1).astype(F32)
    chunk_cols = width // CHUNKS
    fixed_half = (1 << FIXED) - (1 << (FIXED - 4))
    span = chunk_cols // QUARTERS
    group_slices = slices // views

    def tile(chunk, index, carry):
        base = (index * LANES + chunk * chunk_cols).astype(F32) - half
        x_all = lanes + base
        twice_base = 2 * (index * LANES + chunk * chunk_cols) - (width - 1)
        totals = [jnp.zeros((slices, LANES), F32) for _ in range(ROW_DEV)]
        for view in range(view_count):
            cosine = cos_ref[first_view + view]
            sine = sin_ref[first_view + view]
            center = shift_ref[view].astype(F32) + ((bins - 1) / 2.0 + MARGIN)
            along = x_all * cosine
            fixed_cos = fixed_cos_ref[first_view + view]
            fixed_sin = fixed_sin_ref[first_view + view]
            ends = jnp.minimum(twice_base * fixed_cos, (twice_base + 2 * (LANES - 1)) * fixed_cos) + fixed_half
            origin = shift_ref[view] + ((bins - 1) // 2 + MARGIN)
            twice_y = 2 * row_base - (image_rows - 1)
            window = (((ends + twice_y * fixed_sin) >> (FIXED + 1)) + origin) >> 6
            rows = slice(view * slices, (view + 1) * slices)
            low_near, low_far = low_ref[window, rows], low_ref[window + 2, rows]
            high_near, high_far = high_ref[window, rows], high_ref[window + 2, rows]
            for row in range(ROW_DEV):
                y = (row_base + row).astype(F32) - (image_rows - 1) / 2.0
                lift = y * sine
                place = (along + lift) + center
                lower = jnp.floor(place)
                fraction = place - lower
                weight_low = (1.0 - fraction).astype(BF16).astype(F32)
                weight_high = fraction.astype(BF16).astype(F32)
                spot = lower.astype(jnp.int32) - window * WINDOW
                near = spot < LANES
                inner = spot & (LANES - 1)
                take = functools.partial(jnp.take_along_axis, indices=inner, axis=1, mode="promise_in_bounds")
                low = jnp.where(near, take(low_near), take(low_far))
                high = jnp.where(near, take(high_near), take(high_far))
                totals[row] = totals[row] + (low * weight_low + high * weight_high)
        for row in range(ROW_DEV):
            part_ref[row * slices:(row + 1) * slices, pl.ds(pl.multiple_of(index * LANES, LANES), LANES)] = totals[row]
        return carry

    copies = []
    for chunk in range(CHUNKS):
        lax.fori_loop(0, chunk_cols // LANES, functools.partial(tile, chunk), 0)
        gathered = jnp.concatenate([part_ref[:, q * span:(q + 1) * span] for q in range(QUARTERS)], axis=0).astype(BF16)
        send_ref[chunk] = dot(perm_out_ref[...], gathered).astype(BF16).reshape(slices, QUARTERS * ROW_DEV, span)
        if chunk == 0:
            pl.semaphore_wait(barrier, views + 1)
        sent = []
        for step in range(1, views):
            peer = lax.rem(me + step, views)
            slot = chunk * (views - 1) + step - 1
            copy = pltpu.make_async_remote_copy(
                src_ref=send_ref.at[chunk, pl.ds(peer * group_slices, group_slices)], dst_ref=recv_ref.at[slot],
                send_sem=send_sem.at[slot], recv_sem=recv_sem.at[slot],
                device_id={"views": peer}, device_id_type=MESH)
            copy.start()
            sent.append((slot, copy))
        copies.append(sent)

    one, two, second = tap_matrices(conv_one_ref, bias_one_ref, conv_two_ref, bias_two_ref, expand_ref)
    one_ref[...] = one
    two_ref[...] = two
    second_ref[...] = second

    def place_rows(index, chunk, values, first_row, count):
        for row in range(count):
            for q in range(QUARTERS):
                column = chunk * chunk_cols + q * span
                out_ref[index, first_row + row:first_row + row + 1, column:column + span] = (
                    values[row * QUARTERS + q:row * QUARTERS + q + 1])

    rows_half = QUARTERS * ROW_DEV // 2
    halos = []
    for chunk in range(CHUNKS):
        total = send_ref[chunk, pl.ds(me * group_slices, group_slices)].astype(F32)
        for slot, copy in copies[chunk]:
            copy.wait_recv()
            total = total + recv_ref[slot].astype(F32)
        image = (total * scale).astype(BF16).astype(F32)
        own_ref[chunk] = image
        to_above = pltpu.make_async_remote_copy(
            src_ref=own_ref.at[chunk, :, pl.ds(0, rows_half)], dst_ref=down_ref.at[chunk],
            send_sem=halo_send.at[2 * chunk], recv_sem=halo_recv.at[2 * chunk],
            device_id={"rows": above}, device_id_type=MESH)
        to_below = pltpu.make_async_remote_copy(
            src_ref=own_ref.at[chunk, :, pl.ds(rows_half, rows_half)], dst_ref=up_ref.at[chunk],
            send_sem=halo_send.at[2 * chunk + 1], recv_sem=halo_recv.at[2 * chunk + 1],
            device_id={"rows": below}, device_id_type=MESH)
        to_above.start()
        to_below.start()
        halos.append((to_above, to_below))
        for index in range(group_slices):
            place_rows(index, chunk, image[index], 2, ROW_DEV)
    has_above = (group > 0).astype(F32)
    has_below = (group < row_groups - 1).astype(F32)
    for chunk, (to_above, to_below) in enumerate(halos):
        to_above.wait_recv()
        to_below.wait_recv()
        for index in range(group_slices):
            place_rows(index, chunk, up_ref[chunk, index] * has_above, 0, 2)
            place_rows(index, chunk, down_ref[chunk, index] * has_below, 2 + ROW_DEV, 2)
    for sent in copies:
        for _, copy in sent:
            copy.wait_send()
    for pair in halos:
        for copy in pair:
            copy.wait_send()


def conv_kernel(row_groups, rows_ref, one_ref, two_ref, second_ref, out_ref):
    group = lax.axis_index("rows")
    width = rows_ref.shape[2]
    channels = out_ref.shape[1]
    source = rows_ref[0]
    column = lax.broadcasted_iota(jnp.int32, (1, width), 1)

    def spread(values):
        left = jnp.where(column == 0, 0.0, pltpu.roll(values, 1, 1))
        right = jnp.where(column == width - 1, 0.0, pltpu.roll(values, width - 1, 1))
        return [left, values, right]

    window = jnp.concatenate(spread(source), axis=0).astype(BF16)
    window = jnp.concatenate([window] * 3 + [jnp.ones((8, width), BF16)], axis=0)
    hidden = jnp.maximum(dot(one_ref[...], window), 0.0)
    hidden_rows = ROW_DEV + 2
    line = lax.broadcasted_iota(jnp.int32, (hidden_rows * channels, 1), 0)
    lowest = jnp.where(group > 0, 0, channels)
    highest = jnp.where(group < row_groups - 1, hidden_rows * channels, (hidden_rows - 1) * channels)
    hidden = jnp.where((line >= lowest) & (line < highest), hidden, 0.0)
    stacked = jnp.concatenate([piece.astype(BF16) for piece in spread(hidden)], axis=0)
    mixed = jnp.maximum(dot(two_ref[...], stacked) + second_ref[:, :1], 0.0)
    out_ref[0] = mixed.reshape(channels, ROW_DEV, width).astype(BF16)


def local(sinogram, view_shift, conv_one, bias_one, conv_two, bias_two):
    slices, view_count, bins = sinogram.shape
    views = lax.axis_size("views")
    row_groups = lax.axis_size("rows")
    views_total = view_count * views
    image_rows = ROW_DEV * row_groups
    channels = conv_one.shape[1]
    flat = slices * view_count
    group_slices = slices // views
    extended = bins + 2 * MARGIN
    span = bins // (QUARTERS * CHUNKS)

    angles = (np.arange(views_total, dtype=np.float32) * np.float32(math.pi / views_total)).astype(np.float64)
    cosines = jnp.asarray(np.cos(angles).astype(np.float32))
    sines = jnp.asarray(np.sin(angles).astype(np.float32))
    fixed_cosines = jnp.asarray(np.round(np.cos(angles) * (1 << FIXED)).astype(np.int32))
    fixed_sines = jnp.asarray(np.round(np.sin(angles) * (1 << FIXED)).astype(np.int32))
    order = np.arange(flat).reshape(slices, view_count).T.reshape(-1)
    perm_in = np.zeros((flat, flat), np.float32)
    perm_in[np.arange(flat), order] = 1.0
    size = QUARTERS * ROW_DEV * slices
    order = np.arange(size).reshape(QUARTERS, ROW_DEV, slices).transpose(2, 1, 0).reshape(-1)
    perm_out = np.zeros((size, size), np.float32)
    perm_out[np.arange(size), order] = 1.0

    expand = np.repeat(np.eye(channels, dtype=np.float32), ROW_DEV, axis=0)

    vmem = pl.BlockSpec(memory_space=pltpu.VMEM)
    smem = pl.BlockSpec(memory_space=pltpu.SMEM)
    hidden_rows = ROW_DEV + 2
    halo = pltpu.VMEM((CHUNKS, group_slices, QUARTERS * ROW_DEV // 2, span), F32)
    slots = CHUNKS * (views - 1)
    rows, one, two, second = pl.pallas_call(
        functools.partial(project_kernel, views, row_groups),
        out_shape=(
            jax.ShapeDtypeStruct((group_slices, ROW_DEV + 4, bins), F32),
            jax.ShapeDtypeStruct((hidden_rows * channels, 9 * (ROW_DEV + 4) + 8), BF16),
            jax.ShapeDtypeStruct((channels * ROW_DEV, 3 * hidden_rows * channels), BF16),
            jax.ShapeDtypeStruct((channels * ROW_DEV, LANES), F32),
        ),
        in_specs=[vmem] * 4 + [smem] * 5 + [vmem] * 4,
        out_specs=(vmem,) * 4,
        scratch_shapes=[
            pltpu.VMEM((bins // BLOCK * flat, BLOCK), F32),
            pltpu.VMEM((extended // WINDOW, flat, LANES), F32),
            pltpu.VMEM((extended // WINDOW, flat, LANES), F32),
            pltpu.VMEM((ROW_DEV * slices, bins // CHUNKS), F32),
            pltpu.VMEM((CHUNKS, slices, QUARTERS * ROW_DEV, span), BF16),
            pltpu.VMEM((slots, group_slices, QUARTERS * ROW_DEV, span), BF16),
            pltpu.VMEM((CHUNKS, group_slices, QUARTERS * ROW_DEV, span), F32),
            halo,
            halo,
            pltpu.SemaphoreType.DMA((slots,)),
            pltpu.SemaphoreType.DMA((slots,)),
            pltpu.SemaphoreType.DMA((2 * CHUNKS,)),
            pltpu.SemaphoreType.DMA((2 * CHUNKS,)),
        ],
        compiler_params=pltpu.CompilerParams(collective_id=0, has_side_effects=True),
        name="project",
    )(sinogram, jnp.asarray(perm_in, dtype=BF16), jnp.asarray(perm_out, dtype=BF16), jnp.asarray(expand, dtype=BF16),
      view_shift, cosines, sines, fixed_cosines, fixed_sines, conv_one, bias_one[None, :], conv_two, bias_two[None, :])

    conv = pl.pallas_call(
        functools.partial(conv_kernel, row_groups),
        grid=(group_slices,),
        out_shape=jax.ShapeDtypeStruct((group_slices, channels, ROW_DEV, bins), BF16),
        in_specs=[pl.BlockSpec((1, ROW_DEV + 4, bins), lambda i: (i, 0, 0))] + [vmem] * 3,
        out_specs=pl.BlockSpec((1, channels, ROW_DEV, bins), lambda i: (i, 0, 0, 0)),
        name="conv",
    )
    return conv(rows, one, two, second)


def solution(mesh):
    return jax.shard_map(
        local,
        mesh=mesh,
        in_specs=(P(None, "views", None), P("views"), P(), P(), P(), P()),
        out_specs=P("views", None, "rows", None),
        check_vma=False,
    )
```

```python
import functools
import math

import jax
import jax.numpy as jnp
import numpy as np
from jax import lax
from jax.experimental import pallas as pl
from jax.experimental.pallas import tpu as pltpu
from jax.sharding import PartitionSpec as P

MARGIN = 384
ROW_DEV = 4
LANES = 128
BLOCK = 256
QUARTERS = 4
CHUNKS = 4
FIXED = 18
WINDOW = 64
F32 = jnp.float32
BF16 = jnp.bfloat16
MESH = pl.DeviceIdType.MESH


def split_parts(values, count):
    parts = []
    rest = values
    for part in range(count):
        piece = rest.astype(BF16)
        parts.append(piece)
        if part + 1 < count:
            rest = rest - piece.astype(F32)
    return parts


def ramp_base():
    rows = lax.broadcasted_iota(jnp.int32, (BLOCK, BLOCK), 0)
    cols = lax.broadcasted_iota(jnp.int32, (BLOCK, BLOCK), 1)
    offset = cols - rows
    return offset.astype(F32), jnp.where((offset & 1) != 0, -1.0 / (math.pi * math.pi), 0.0)


def ramp_block(base, numerator, block_offset):
    offset = base + float(block_offset * BLOCK)
    square = offset * offset
    if block_offset == 0:
        return jnp.where(base == 0.0, 0.25, numerator / jnp.maximum(square, 1.0))
    return numerator / square


def dot(a, b):
    return lax.dot_general(a, b, (((1,), (0,)), ((), ())), preferred_element_type=F32)


def dot_t(a, b):
    return lax.dot_general(a, b, (((1,), (1,)), ((), ())), preferred_element_type=F32)


def tap_matrices(one_ref, bias_one_ref, two_ref, bias_two_ref, expand_ref):
    channels = one_ref.shape[1]
    hidden_rows = ROW_DEV + 2
    image_lines = ROW_DEV + 4
    lanes = hidden_rows * channels
    rep = jnp.concatenate([one_ref[...]] * hidden_rows, axis=1)
    line = lax.broadcasted_iota(jnp.int32, (3 * image_lines, lanes), 0) % image_lines
    target = lax.broadcasted_iota(jnp.int32, (3 * image_lines, lanes), 1) // channels
    full = jnp.zeros((3 * image_lines, lanes), F32)
    for i in range(3):
        picked = jnp.concatenate(
            [jnp.broadcast_to(rep[3 * i + dx:3 * i + dx + 1], (image_lines, lanes)) for dx in range(3)], axis=0)
        full = full + jnp.where(line - target == i, picked, 0.0)
    bias = jnp.concatenate([bias_one_ref[...]] * hidden_rows, axis=1)
    bias_parts = [piece.astype(F32) for piece in split_parts(bias, 3)]
    bias_rows = jnp.concatenate(bias_parts + [jnp.zeros((5, lanes), F32)], axis=0)
    pieces = [piece.astype(F32) for piece in split_parts(full, 3)]
    one = jnp.concatenate(pieces + [bias_rows], axis=0).T.astype(BF16)
    taps = two_ref[...].astype(F32)
    depth = 3 * hidden_rows * channels
    rows = channels * ROW_DEV
    out_row = lax.broadcasted_iota(jnp.int32, (rows, depth), 0) % ROW_DEV
    hidden_row = (lax.broadcasted_iota(jnp.int32, (rows, depth), 1) // channels) % hidden_rows
    two = jnp.zeros((rows, depth), F32)
    for i in range(3):
        wide = jnp.concatenate(
            [taps[:, (3 * i + dx) * channels:(3 * i + dx + 1) * channels] for dx in range(3) for _ in range(hidden_rows)],
            axis=1)
        two = two + jnp.where(hidden_row - out_row == i, dot(expand_ref[...], wide.astype(BF16)), 0.0)
    second = sum(dot_t(expand_ref[...], jnp.broadcast_to(piece.astype(F32), (LANES, channels)).astype(BF16))
                 for piece in split_parts(bias_two_ref[...], 3))
    return one, two.astype(BF16), second


def project_kernel(views, row_groups, sino_ref, perm_in_ref, perm_out_ref, expand_ref, shift_ref, cos_ref, sin_ref, fixed_cos_ref, fixed_sin_ref,
                   conv_one_ref, bias_one_ref, conv_two_ref, bias_two_ref,
                   out_ref, one_ref, two_ref, second_ref,
                   sum_ref, low_ref, high_ref, part_ref, send_ref, recv_ref, own_ref, up_ref, down_ref,
                   send_sem, recv_sem, halo_send, halo_recv):
    me = lax.axis_index("views")
    group = lax.axis_index("rows")
    above = lax.rem(group + row_groups - 1, row_groups)
    below = lax.rem(group + 1, row_groups)
    barrier = pltpu.get_barrier_semaphore()
    for step in range(1, views):
        pl.semaphore_signal(barrier, inc=1, device_id={"views": lax.rem(me + step, views)}, device_id_type=MESH)
    for other in (above, below):
        pl.semaphore_signal(barrier, inc=1, device_id={"rows": other}, device_id_type=MESH)

    slices, view_count, bins = sino_ref.shape
    width = bins
    flat = slices * view_count
    blocks = bins // BLOCK
    views_total = view_count * views
    image_rows = ROW_DEV * row_groups
    scale = math.pi / views_total
    ordered = dot(perm_in_ref[...], sino_ref[...].reshape(flat, bins)).astype(BF16)
    stacked = jnp.concatenate([ordered[:, k * BLOCK:(k + 1) * BLOCK] for k in range(blocks)], axis=0)
    base_offset, numerator = ramp_base()
    for step in range(blocks):
        parts = split_parts(ramp_block(base_offset, numerator, step), 3 if step < 2 else 1)
        count = (blocks - step) * flat
        down = stacked[:count]
        forward = sum(dot(down, part) for part in parts[::-1])
        if step == 0:
            sum_ref[...] = forward
        else:
            sum_ref[pl.ds(step * flat, count), :] += forward
            up = stacked[step * flat:]
            backward = sum(dot_t(up, part) for part in parts[::-1])
            sum_ref[pl.ds(0, count), :] += backward
    zeros = jnp.zeros((flat, MARGIN), F32)
    filtered = [sum_ref[k * flat:(k + 1) * flat, :].astype(BF16).astype(F32) for k in range(blocks)]
    padded = jnp.concatenate([zeros] + filtered + [zeros], axis=1)
    for ref, lead in ((low_ref, 0), (high_ref, 1)):
        for odd in range(2):
            turn = odd * WINDOW + lead
            turned = pltpu.roll(padded, padded.shape[1] - turn, 1) if turn else padded
            for block in range(ref.shape[0] // 2):
                ref[2 * block + odd] = turned[:, block * LANES:(block + 1) * LANES]

    first_view = me * view_count
    row_base = group * ROW_DEV
    half = (width - 1) / 2.0
    lanes = lax.broadcasted_iota(jnp.int32, (slices, LANES), 1).astype(F32)
    chunk_cols = width // CHUNKS
    fixed_half = (1 << FIXED) - (1 << (FIXED - 4))
    span = chunk_cols // QUARTERS
    group_slices = slices // views

    def tile(chunk, index, carry):
        base = (index * LANES + chunk * chunk_cols).astype(F32) - half
        x_all = lanes + base
        twice_base = 2 * (index * LANES + chunk * chunk_cols) - (width - 1)
        totals = [jnp.zeros((slices, LANES), F32) for _ in range(ROW_DEV)]
        for view in range(view_count):
            cosine = cos_ref[first_view + view]
            sine = sin_ref[first_view + view]
            center = shift_ref[view].astype(F32) + ((bins - 1) / 2.0 + MARGIN)
            along = x_all * cosine
            fixed_cos = fixed_cos_ref[first_view + view]
            fixed_sin = fixed_sin_ref[first_view + view]
            ends = jnp.minimum(twice_base * fixed_cos, (twice_base + 2 * (LANES - 1)) * fixed_cos) + fixed_half
            origin = shift_ref[view] + ((bins - 1) // 2 + MARGIN)
            twice_y = 2 * row_base - (image_rows - 1)
            window = (((ends + twice_y * fixed_sin) >> (FIXED + 1)) + origin) >> 6
            rows = slice(view * slices, (view + 1) * slices)
            low_near, low_far = low_ref[window, rows], low_ref[window + 2, rows]
            high_near, high_far = high_ref[window, rows], high_ref[window + 2, rows]
            for row in range(ROW_DEV):
                y = (row_base + row).astype(F32) - (image_rows - 1) / 2.0
                lift = y * sine
                place = (along + lift) + center
                lower = jnp.floor(place)
                fraction = place - lower
                weight_low = (1.0 - fraction).astype(BF16).astype(F32)
                weight_high = fraction.astype(BF16).astype(F32)
                spot = lower.astype(jnp.int32) - window * WINDOW
                near = spot < LANES
                inner = spot & (LANES - 1)
                take = functools.partial(jnp.take_along_axis, indices=inner, axis=1, mode="promise_in_bounds")
                low = jnp.where(near, take(low_near), take(low_far))
                high = jnp.where(near, take(high_near), take(high_far))
                totals[row] = totals[row] + (low * weight_low + high * weight_high)
        for row in range(ROW_DEV):
            part_ref[row * slices:(row + 1) * slices, pl.ds(pl.multiple_of(index * LANES, LANES), LANES)] = totals[row]
        return carry

    copies = []
    for chunk in range(CHUNKS):
        lax.fori_loop(0, chunk_cols // LANES, functools.partial(tile, chunk), 0)
        gathered = jnp.concatenate([part_ref[:, q * span:(q + 1) * span] for q in range(QUARTERS)], axis=0).astype(BF16)
        send_ref[chunk] = dot(perm_out_ref[...], gathered).astype(BF16).reshape(slices, QUARTERS * ROW_DEV, span)
        if chunk == 0:
            pl.semaphore_wait(barrier, views + 1)
        sent = []
        for step in range(1, views):
            peer = lax.rem(me + step, views)
            slot = chunk * (views - 1) + step - 1
            copy = pltpu.make_async_remote_copy(
                src_ref=send_ref.at[chunk, pl.ds(peer * group_slices, group_slices)], dst_ref=recv_ref.at[slot],
                send_sem=send_sem.at[slot], recv_sem=recv_sem.at[slot],
                device_id={"views": peer}, device_id_type=MESH)
            copy.start()
            sent.append((slot, copy))
        copies.append(sent)

    one, two, second = tap_matrices(conv_one_ref, bias_one_ref, conv_two_ref, bias_two_ref, expand_ref)
    one_ref[...] = one
    two_ref[...] = two
    second_ref[...] = second

    def place_rows(index, chunk, values, first_row, count):
        for row in range(count):
            for q in range(QUARTERS):
                column = chunk * chunk_cols + q * span
                out_ref[index, first_row + row:first_row + row + 1, column:column + span] = (
                    values[row * QUARTERS + q:row * QUARTERS + q + 1])

    rows_half = QUARTERS * ROW_DEV // 2
    halos = []
    for chunk in range(CHUNKS):
        total = send_ref[chunk, pl.ds(me * group_slices, group_slices)].astype(F32)
        for slot, copy in copies[chunk]:
            copy.wait_recv()
            total = total + recv_ref[slot].astype(F32)
        image = (total * scale).astype(BF16).astype(F32)
        own_ref[chunk] = image
        to_above = pltpu.make_async_remote_copy(
            src_ref=own_ref.at[chunk, :, pl.ds(0, rows_half)], dst_ref=down_ref.at[chunk],
            send_sem=halo_send.at[2 * chunk], recv_sem=halo_recv.at[2 * chunk],
            device_id={"rows": above}, device_id_type=MESH)
        to_below = pltpu.make_async_remote_copy(
            src_ref=own_ref.at[chunk, :, pl.ds(rows_half, rows_half)], dst_ref=up_ref.at[chunk],
            send_sem=halo_send.at[2 * chunk + 1], recv_sem=halo_recv.at[2 * chunk + 1],
            device_id={"rows": below}, device_id_type=MESH)
        to_above.start()
        to_below.start()
        halos.append((to_above, to_below))
        for index in range(group_slices):
            place_rows(index, chunk, image[index], 2, ROW_DEV)
    has_above = (group > 0).astype(F32)
    has_below = (group < row_groups - 1).astype(F32)
    for chunk, (to_above, to_below) in enumerate(halos):
        to_above.wait_recv()
        to_below.wait_recv()
        for index in range(group_slices):
            place_rows(index, chunk, up_ref[chunk, index] * has_above, 0, 2)
            place_rows(index, chunk, down_ref[chunk, index] * has_below, 2 + ROW_DEV, 2)
    for sent in copies:
        for _, copy in sent:
            copy.wait_send()
    for pair in halos:
        for copy in pair:
            copy.wait_send()


def conv_kernel(row_groups, rows_ref, one_ref, two_ref, second_ref, out_ref):
    group = lax.axis_index("rows")
    width = rows_ref.shape[2]
    channels = out_ref.shape[1]
    source = rows_ref[0]
    column = lax.broadcasted_iota(jnp.int32, (1, width), 1)

    def spread(values):
        left = jnp.where(column == 0, 0.0, pltpu.roll(values, 1, 1))
        right = jnp.where(column == width - 1, 0.0, pltpu.roll(values, width - 1, 1))
        return [left, values, right]

    window = jnp.concatenate(spread(source), axis=0).astype(BF16)
    window = jnp.concatenate([window] * 3 + [jnp.ones((8, width), BF16)], axis=0)
    hidden = jnp.maximum(dot(one_ref[...], window), 0.0)
    hidden_rows = ROW_DEV + 2
    line = lax.broadcasted_iota(jnp.int32, (hidden_rows * channels, 1), 0)
    lowest = jnp.where(group > 0, 0, channels)
    highest = jnp.where(group < row_groups - 1, hidden_rows * channels, (hidden_rows - 1) * channels)
    hidden = jnp.where((line >= lowest) & (line < highest), hidden, 0.0)
    stacked = jnp.concatenate([piece.astype(BF16) for piece in spread(hidden)], axis=0)
    mixed = jnp.maximum(dot(two_ref[...], stacked) + second_ref[:, :1], 0.0)
    out_ref[0] = mixed.reshape(channels, ROW_DEV, width).astype(BF16)


def local(sinogram, view_shift, conv_one, bias_one, conv_two, bias_two):
    slices, view_count, bins = sinogram.shape
    views = lax.axis_size("views")
    row_groups = lax.axis_size("rows")
    views_total = view_count * views
    image_rows = ROW_DEV * row_groups
    channels = conv_one.shape[1]
    flat = slices * view_count
    group_slices = slices // views
    extended = bins + 2 * MARGIN
    span = bins // (QUARTERS * CHUNKS)

    angles = (np.arange(views_total, dtype=np.float32) * np.float32(math.pi / views_total)).astype(np.float64)
    cosines = jnp.asarray(np.cos(angles).astype(np.float32))
    sines = jnp.asarray(np.sin(angles).astype(np.float32))
    fixed_cosines = jnp.asarray(np.round(np.cos(angles) * (1 << FIXED)).astype(np.int32))
    fixed_sines = jnp.asarray(np.round(np.sin(angles) * (1 << FIXED)).astype(np.int32))
    order = np.arange(flat).reshape(slices, view_count).T.reshape(-1)
    perm_in = np.zeros((flat, flat), np.float32)
    perm_in[np.arange(flat), order] = 1.0
    size = QUARTERS * ROW_DEV * slices
    order = np.arange(size).reshape(QUARTERS, ROW_DEV, slices).transpose(2, 1, 0).reshape(-1)
    perm_out = np.zeros((size, size), np.float32)
    perm_out[np.arange(size), order] = 1.0

    expand = np.repeat(np.eye(channels, dtype=np.float32), ROW_DEV, axis=0)

    vmem = pl.BlockSpec(memory_space=pltpu.VMEM)
    smem = pl.BlockSpec(memory_space=pltpu.SMEM)
    hidden_rows = ROW_DEV + 2
    halo = pltpu.VMEM((CHUNKS, group_slices, QUARTERS * ROW_DEV // 2, span), F32)
    slots = CHUNKS * (views - 1)
    rows, one, two, second = pl.pallas_call(
        functools.partial(project_kernel, views, row_groups),
        out_shape=(
            jax.ShapeDtypeStruct((group_slices, ROW_DEV + 4, bins), F32),
            jax.ShapeDtypeStruct((hidden_rows * channels, 9 * (ROW_DEV + 4) + 8), BF16),
            jax.ShapeDtypeStruct((channels * ROW_DEV, 3 * hidden_rows * channels), BF16),
            jax.ShapeDtypeStruct((channels * ROW_DEV, LANES), F32),
        ),
        in_specs=[vmem] * 4 + [smem] * 5 + [vmem] * 4,
        out_specs=(vmem,) * 4,
        scratch_shapes=[
            pltpu.VMEM((bins // BLOCK * flat, BLOCK), F32),
            pltpu.VMEM((extended // WINDOW, flat, LANES), F32),
            pltpu.VMEM((extended // WINDOW, flat, LANES), F32),
            pltpu.VMEM((ROW_DEV * slices, bins // CHUNKS), F32),
            pltpu.VMEM((CHUNKS, slices, QUARTERS * ROW_DEV, span), BF16),
            pltpu.VMEM((slots, group_slices, QUARTERS * ROW_DEV, span), BF16),
            pltpu.VMEM((CHUNKS, group_slices, QUARTERS * ROW_DEV, span), F32),
            halo,
            halo,
            pltpu.SemaphoreType.DMA((slots,)),
            pltpu.SemaphoreType.DMA((slots,)),
            pltpu.SemaphoreType.DMA((2 * CHUNKS,)),
            pltpu.SemaphoreType.DMA((2 * CHUNKS,)),
        ],
        compiler_params=pltpu.CompilerParams(collective_id=0, has_side_effects=True),
        name="project",
    )(sinogram, jnp.asarray(perm_in, dtype=BF16), jnp.asarray(perm_out, dtype=BF16), jnp.asarray(expand, dtype=BF16),
      view_shift, cosines, sines, fixed_cosines, fixed_sines, conv_one, bias_one[None, :], conv_two, bias_two[None, :])

    conv = pl.pallas_call(
        functools.partial(conv_kernel, row_groups),
        grid=(group_slices,),
        out_shape=jax.ShapeDtypeStruct((group_slices, channels, ROW_DEV, bins), BF16),
        in_specs=[pl.BlockSpec((1, ROW_DEV + 4, bins), lambda i: (i, 0, 0))] + [vmem] * 3,
        out_specs=pl.BlockSpec((1, channels, ROW_DEV, bins), lambda i: (i, 0, 0, 0)),
        name="conv",
    )
    return conv(rows, one, two, second)


def solution(mesh):
    return jax.shard_map(
        local,
        mesh=mesh,
        in_specs=(P(None, "views", None), P("views"), P(), P(), P(), P()),
        out_specs=P("views", None, "rows", None),
        check_vma=False,
    )
```
